256 devices in a mesh: seq: 32 (over z, x_lo, core), fsdp: 8 (over x_hi, y).
Axes of the slice: x: 4 (x_hi: 2, x_lo: 2; x = x_hi * 2 + x_lo), y: 4, z: 8, core: 2. Of those that a mesh axis runs over, the one named last changes fastest.
Arguments:
- hidden_next: bfloat16 [8192, 8192], P('seq'), may hold values from -6 to 6
- values_next: bfloat16 [8192, 8192], P('seq', 'fsdp'), may hold values from -6 to 6
- seg_next: int32 [4], replicated, may hold values from 1 to 4096, 8192 in all
- proj_bc: bfloat16 [8192, 1024], P(('seq', 'fsdp')), may hold values from -0.09375 to 0.09375
- proj_dt: bfloat16 [8192, 128], P(('seq', 'fsdp')), may hold values from -0.0625 to 0.0625
- dt_bias: float32 [128], replicated, may hold values from -4 to -2.5
- decay_rate: float32 [128], replicated, may hold values from 0 to 1, as said below
- skip_gain: float32 [128], replicated, may hold values from 0.5 to 1.5
- bc_prev: bfloat16 [8192, 1024], P('seq'), may hold values from -4 to 4
- dt_prev: float32 [8192, 128], P('seq', 'fsdp'), may hold values from 0.01 to 0.3
- seg_prev: int32 [4], replicated, may hold values from 1 to 4096, 8192 in all
- grad_prev: bfloat16 [8192, 8192], P('seq', 'fsdp'), may hold values from -6 to 6
Outputs:
- out_next: bfloat16 [8192, 8192], P('seq', 'fsdp')
- grad_values: bfloat16 [8192, 8192], P('seq', 'fsdp')
The draws below stay inside these ranges and needn't reach their ends.
Inputs may be any that keep to these rules, and one draw needn't show every extreme that they name: `seg_next`: lengths of the rollout's 4 segments in order, summing to 8192. `seg_prev`: lengths of the rollout's 4 segments in order, summing to 8192. `decay_rate`: positive.
All inputs are finite; a program needn't handle non-finite values.
Results may differ from the reference program's by a relative error of at most 0.0064.
Values may be sent and summed in bfloat16 or wider, within the bound.
A program may use at most 128 MiB of HBM per device.

```python
import math
import jax
import jax.numpy as jnp
import numpy as np
from jax import lax

D = 8192
HW = 128
P_SIZE = 64
GW = 4
N = 128
SPAN = 128
NSEG = 4
SEQ_LEN = 8192
BCW = 1024


def draw_decay_rate(key, part):
    streams = jax.random.split(jax.random.fold_in(key, 11), 3)
    lasting = jax.random.uniform(streams[0], (HW,)) < 0.5
    slow_rate = jnp.exp(jax.random.uniform(streams[1], (HW,), minval=jnp.log(5.0), maxval=jnp.log(20.0))) / SEQ_LEN
    fast_rate = jnp.exp(jax.random.uniform(streams[2], (HW,), minval=jnp.log(0.25), maxval=jnp.log(0.8)))
    return jnp.where(lasting, slow_rate, fast_rate).astype(jnp.float32)


def spiked(values, stream_key, source, target, blocks, factor):
    owner, partner = [(jnp.arange(values.shape[position]) // (values.shape[position] // blocks)).reshape([-1 if axis == position else 1 for axis in range(values.ndim)]) for position in (source, target)]
    chosen = jax.random.permutation(stream_key, blocks)[partner]
    strong = (owner == chosen) | (owner == (partner + blocks // 2) % blocks)
    return jnp.where(strong, factor * values, values)


def block_scale(rng, shape, cuts, least, largest):
    def one(axis_at, shards_of):
        heights = jax.random.uniform(jax.random.fold_in(jax.random.fold_in(rng, 6), axis_at), (shards_of,), jnp.float32, least / len(cuts), largest / len(cuts))
        return jnp.repeat(jnp.exp(heights), shape[axis_at] // shards_of).reshape((-1,) + (1,) * (len(shape) - axis_at - 1))

    factor_of = one(*cuts[0])
    for cut in cuts[1:]:
        factor_of = factor_of * one(*cut)
    return factor_of


def split_up(amount, total, reach, lean):
    loads = [(1 << 20) // math.isqrt(rank ** lean) + 1 for rank in range(2, amount + 1)]
    rest, counts = total - reach - (amount - 1), [1] * (amount - 1)
    while rest > 0:
        free = [i for i in range(amount - 1) if counts[i] < reach]
        pool, left = sum([loads[i] for i in free]), rest
        for i in free:
            extra = min(reach - counts[i], max(1, left * loads[i] // pool), rest)
            counts[i] = counts[i] + extra
            rest = rest - extra
    return np.array([reach] + counts)


def uneven(stream_key, count, total, limit, slope):
    if count == 2:
        one = jax.random.randint(stream_key, (), max(1, total - limit), min(limit, total - 1) + 1)
        return jnp.stack([one, total - one])
    sizes = jnp.asarray(split_up(count, total, limit, slope), jnp.int32)
    pairs = (count - 1) // 2
    donor, sink = sizes[1:1 + 2 * pairs:2], sizes[2:2 + 2 * pairs:2]
    slack = jnp.minimum(donor - 1, limit - sink)
    shifted = jax.random.randint(jax.random.fold_in(stream_key, 1), (pairs,), 0, 1 << 20) % (slack + 1)
    sizes = sizes.at[1:1 + 2 * pairs:2].set(donor - shifted).at[2:2 + 2 * pairs:2].set(sink + shifted)
    return sizes[jax.random.permutation(jax.random.fold_in(stream_key, 2), count)]


def noise(own_key, shape, scale, most, pieces=(), kind=jnp.bfloat16):
    factor_of = block_scale(own_key, shape, pieces, -0.22, 0.18) if pieces else 1.0
    drawn = jax.random.normal(own_key, shape, jnp.float32) * scale * factor_of
    return jnp.minimum(jnp.maximum(drawn, -most), most).astype(kind)


def bell_draw_with(stream_key, extent, width, most, cuts, heavy, held_as=jnp.bfloat16):
    entries = width * jax.random.normal(stream_key, extent, jnp.float32)
    if cuts:
        entries = entries * block_scale(stream_key, extent, cuts, -0.22, 0.18)
    return jnp.clip(spiked(entries, jax.random.fold_in(stream_key, 3), *heavy), -most, most).astype(held_as)


def setup_inputs(seed: int = 0) -> dict:
    splits = jax.random.split(jax.random.key(seed), 13)
    hidden_next = noise(splits[0], (SEQ_LEN, D), 1.0, 6.0, ((0, 32),))
    values_next = noise(splits[1], (SEQ_LEN, HW * P_SIZE), 1.0, 6.0, ((0, 32), (1, 8)))
    seg_next = uneven(splits[2], NSEG, SEQ_LEN, SEQ_LEN // 2, 2).astype(jnp.int32)
    proj_bc = bell_draw_with(splits[3], (D, BCW), (D * 8) ** -0.5, 0.09375, ((0, 256),), (0, 1, 256, 6.0))
    proj_dt = noise(splits[4], (D, HW), D ** -0.5, 0.0625, ((0, 256),))
    dt_bias = jnp.clip(jax.random.uniform(splits[5], (HW,), jnp.float32, -4.0, -2.5), -4.0, -2.5)
    decay_rate = draw_decay_rate(jax.random.fold_in(splits[12], 71), 0)
    skip_gain = jnp.clip(jax.random.uniform(splits[7], (HW,), jnp.float32, 0.5, 1.5), 0.5, 1.5)
    bc_prev = noise(splits[8], (SEQ_LEN, BCW), 0.3, 4.0, ((0, 32),))
    dt_prev = jnp.clip(jnp.exp(math.log(0.3) - 3.4011974 * jax.random.uniform(splits[9], (SEQ_LEN, HW), jnp.float32) ** block_scale(splits[9], (SEQ_LEN, HW), ((0, 32), (1, 8)), -0.2, 0.2)), 0.01, 0.3)
    seg_prev = uneven(splits[10], NSEG, SEQ_LEN, SEQ_LEN // 2, 2).astype(jnp.int32)
    grad_prev = noise(splits[11], (SEQ_LEN, HW * P_SIZE), 1.0, 6.0, ((0, 32), (1, 8)))
    return dict(hidden_next=hidden_next, values_next=values_next, seg_next=seg_next, proj_bc=proj_bc, proj_dt=proj_dt, dt_bias=dt_bias, decay_rate=decay_rate, skip_gain=skip_gain, bc_prev=bc_prev, dt_prev=dt_prev, seg_prev=seg_prev, grad_prev=grad_prev)


def segment_table(lengths, tokens_total):
    bounds = jnp.cumsum(lengths)[:-1].astype(jnp.int32)
    places = jnp.arange(tokens_total + 1, dtype=jnp.int32) - 1
    return jnp.sum((bounds[None, :] <= places[:, None]).astype(jnp.int32), axis=1)


def block_parts(bc_block, dt_block, seg_ext, decay_rate):
    span_len = bc_block.shape[0]
    half_cols = bc_block.shape[1] // 2
    b_vectors = bc_block[:, :half_cols].reshape(span_len, GW, N)
    c_vectors = bc_block[:, half_cols:].reshape(span_len, GW, N)
    before = seg_ext[0]
    segment = seg_ext[1:]
    cumulative = jnp.cumsum(-dt_block * decay_rate[None, :], axis=0)
    final_cum = cumulative[-1]
    places = jnp.arange(span_len)
    linked = (segment[:, None] == segment[None, :]) & (places[:, None] >= places[None, :])
    scores = jnp.einsum("tgn,sgn->gts", c_vectors.astype(jnp.float32), b_vectors.astype(jnp.float32),
                        precision=lax.Precision.HIGHEST)
    by_head = cumulative.T
    spread = by_head[:, :, None] - by_head[:, None, :]
    decays = jnp.exp(jnp.where(linked[None], spread, -jnp.inf))
    weighted = (decays * dt_block.T[:, None, :]).reshape(GW, HW // GW, span_len, span_len)
    mixing = (weighted * scores[:, None]).reshape(HW, span_len, span_len).astype(jnp.bfloat16)
    keep_final = (segment == segment[-1]).astype(jnp.float32)
    linked_in = (segment == before).astype(jnp.float32)
    send_factor = keep_final[:, None] * jnp.exp(final_cum[None, :] - cumulative) * dt_block
    read_factor = linked_in[:, None] * jnp.exp(cumulative)
    carry_decay = (segment[-1] == before).astype(jnp.float32) * jnp.exp(final_cum)
    return b_vectors, c_vectors, mixing, send_factor, read_factor, carry_decay


def outer_sum(values, vectors):
    span_len, heads_all, head_dim = values.shape
    grouped = values.reshape(span_len, GW, heads_all // GW, head_dim).astype(jnp.float32)
    result = jnp.einsum("sgqp,sgn->gqpn", grouped, vectors.astype(jnp.float32), precision=lax.Precision.HIGHEST)
    return result.reshape(heads_all, head_dim, vectors.shape[2])


def read_state(state_now, vectors, factor):
    heads_all, head_dim, state_dim = state_now.shape
    grouped = state_now.reshape(GW, heads_all // GW, head_dim, state_dim)
    result = jnp.einsum("gqpn,tgn->tgqp", grouped, vectors.astype(jnp.float32), precision=lax.Precision.HIGHEST)
    return result.reshape(vectors.shape[0], heads_all, head_dim) * factor[:, :, None]


def forward_rollout(hidden, inputs, lengths, proj_bc, proj_dt, dt_bias, decay_rate, skip_gain):
    dt_all = jax.nn.softplus(jnp.dot(hidden, proj_dt, preferred_element_type=jnp.float32) + dt_bias[None, :])
    bc_all = jnp.dot(hidden, proj_bc, preferred_element_type=jnp.float32).astype(jnp.bfloat16)
    seg_all = segment_table(lengths, SEQ_LEN)

    def advance(state_now, block_id):
        offset = (block_id * SPAN).astype(jnp.int32)
        bc_block = lax.dynamic_slice_in_dim(bc_all, offset, SPAN, 0)
        dt_block = lax.dynamic_slice_in_dim(dt_all, offset, SPAN, 0)
        seg_ext = lax.dynamic_slice_in_dim(seg_all, offset, SPAN + 1, 0)
        values = lax.dynamic_slice_in_dim(inputs, offset, SPAN, 0).reshape(SPAN, HW, P_SIZE)
        b_vectors, c_vectors, mixing, send_factor, read_factor, carry_decay = block_parts(
            bc_block, dt_block, seg_ext, decay_rate)
        inside = jnp.einsum("hts,shp->thp", mixing.astype(jnp.float32), values.astype(jnp.float32),
                            precision=lax.Precision.HIGHEST)
        output = inside + read_state(state_now, c_vectors, read_factor) + skip_gain[None, :, None] * values.astype(jnp.float32)
        scaled = (values.astype(jnp.float32) * send_factor[:, :, None]).astype(jnp.bfloat16)
        state_next = carry_decay[:, None, None] * state_now + outer_sum(scaled, b_vectors)
        return state_next, output.astype(jnp.bfloat16).reshape(SPAN, HW * P_SIZE)

    blocks_all = jnp.arange(SEQ_LEN // SPAN, dtype=jnp.int32)
    _, outputs = lax.scan(advance, jnp.zeros((HW, P_SIZE, N), jnp.float32), blocks_all)
    return outputs.reshape(SEQ_LEN, HW * P_SIZE)


def backward_rollout(bc_all, dt_all, lengths, grads_all, decay_rate, skip_gain):
    seg_all = segment_table(lengths, SEQ_LEN)

    def retreat(state_now, block_id):
        offset = (block_id * SPAN).astype(jnp.int32)
        bc_block = lax.dynamic_slice_in_dim(bc_all, offset, SPAN, 0)
        dt_block = lax.dynamic_slice_in_dim(dt_all, offset, SPAN, 0)
        seg_ext = lax.dynamic_slice_in_dim(seg_all, offset, SPAN + 1, 0)
        grad_block = lax.dynamic_slice_in_dim(grads_all, offset, SPAN, 0).reshape(SPAN, HW, P_SIZE)
        b_vectors, c_vectors, mixing, send_factor, read_factor, carry_decay = block_parts(
            bc_block, dt_block, seg_ext, decay_rate)
        inside = jnp.einsum("hts,thp->shp", mixing.astype(jnp.float32), grad_block.astype(jnp.float32),
                            precision=lax.Precision.HIGHEST)
        output = inside + read_state(state_now, b_vectors, send_factor) + skip_gain[None, :, None] * grad_block.astype(jnp.float32)
        scaled = (grad_block.astype(jnp.float32) * read_factor[:, :, None]).astype(jnp.bfloat16)
        state_next = carry_decay[:, None, None] * state_now + outer_sum(scaled, c_vectors)
        return state_next, output.astype(jnp.bfloat16).reshape(SPAN, HW * P_SIZE)

    blocks_all = jnp.arange(SEQ_LEN // SPAN, dtype=jnp.int32)
    _, outputs = lax.scan(retreat, jnp.zeros((HW, P_SIZE, N), jnp.float32), blocks_all, reverse=True)
    return outputs.reshape(SEQ_LEN, HW * P_SIZE)


def reference(hidden_next, values_next, seg_next, proj_bc, proj_dt, dt_bias, decay_rate, skip_gain,
              bc_prev, dt_prev, seg_prev, grad_prev):
    out_next = forward_rollout(hidden_next, values_next, seg_next, proj_bc, proj_dt, dt_bias, decay_rate, skip_gain)
    grad_values = backward_rollout(bc_prev, dt_prev, seg_prev, grad_prev, decay_rate, skip_gain)
    return out_next, grad_values
```

```python
import functools

import jax
import jax.numpy as jnp
from jax import lax
from jax.experimental import pallas as pl
from jax.experimental.pallas import tpu as pltpu
from jax.sharding import Mesh
from jax.sharding import PartitionSpec as P

MESH = pl.DeviceIdType.MESH
SEQ = ("z", "xl", "c")
FSDP = ("xh", "y")
F32, BF16, I32 = jnp.float32, jnp.bfloat16, jnp.int32
NZ, NSLAB = 8, 32
SPAN, HEADS, WIDE = 128, 16, 1024
TOKENS = 256
VMEM = pl.BlockSpec(memory_space=pltpu.VMEM)
SMEM = pl.BlockSpec(memory_space=pltpu.SMEM)
ANY = pl.BlockSpec(memory_space=pl.ANY)


def iota(shape, dim):
    return lax.broadcasted_iota(I32, shape, dim)


def place():
    z, xl, c = lax.axis_index("z"), lax.axis_index("xl"), lax.axis_index("c")
    xh, y = lax.axis_index("xh"), lax.axis_index("y")
    return z, xl, c, xh, y


def dot(a, b, ca, cb):
    return lax.dot_general(a, b, (((ca,), (cb,)), ((), ())), preferred_element_type=F32)


def split3(v):
    hi = v.astype(BF16)
    rest = v - hi.astype(F32)
    mid = rest.astype(BF16)
    low = (rest - mid.astype(F32)).astype(BF16)
    return jnp.concatenate([hi, mid, low], axis=0)


def spread_matrix(shift):
    n = HEADS << shift
    same = (iota((48, n), 0) & 15) == (iota((48, n), 1) >> shift)
    return jnp.where(same, 1.0, 0.0).astype(BF16)


def per_head_column(row, scratch, first_head):
    scratch[...] = jnp.broadcast_to(row, (128, 128)).T
    return scratch[pl.ds(pl.multiple_of(first_head, HEADS), HEADS), :]


def segment_of(bounds, places):
    count = [jnp.where(places >= b, 1, 0).astype(I32) for b in bounds]
    return count[0] + count[1] + count[2]


def scalar_segment(bounds, position):
    count = [(position >= b).astype(I32) for b in bounds]
    return count[0] + count[1] + count[2]


def local_math(back, bvec, cvec, dt, rate, skip, x_ref, bounds, first, outs):
    pieces, decay, base, factor, inner, carry_row = outs
    wide = spread_matrix(6)
    tall = spread_matrix(7)
    rows, cols = iota((SPAN, SPAN), 0), iota((SPAN, SPAN), 1)
    upper = jnp.where(rows <= cols, 1.0, 0.0).astype(BF16)
    left_half = cols < 64
    sums, carries = [], []
    for blk in range(2):
        sl = slice(SPAN * blk, SPAN * blk + SPAN)
        b_blk, c_blk = bvec(blk), cvec(blk)
        dt_blk = dt[:, sl]
        parts = dot(split3(-(dt_blk * rate)), upper, 1, 0)
        cum = parts[0:16] + (parts[16:32] + parts[32:48])
        start = first + SPAN * blk
        mask = (segment_of(bounds, start + rows) == segment_of(bounds, start + cols)) & (rows >= cols)
        seg_end = scalar_segment(bounds, start + (SPAN - 1))
        seg_before = scalar_segment(bounds, start - 1)
        seg_row = segment_of(bounds, start + iota((HEADS, SPAN), 1))
        cum_end = jnp.broadcast_to(cum[:, SPAN - 1 : SPAN], (HEADS, SPAN))
        send = jnp.where(seg_row == seg_end, jnp.exp(cum_end - cum) * dt_blk, 0.0)
        read = jnp.where(seg_row == seg_before, jnp.exp(cum), 0.0)
        through = jnp.where(seg_end == seg_before, 1.0, 0.0)
        carry = jnp.exp(cum_end) * through
        both = dot(split3(jnp.where(iota((HEADS, SPAN), 1) < 64, carry, skip)), wide, 0, 0)
        carry_x, skip_x = both[0:8], both[64:65]
        scale_x = dot(split3(read if back else send), wide, 0, 0)
        factor[:, sl] = send if back else read
        sent = (x_ref[sl, :].astype(F32) * scale_x).astype(BF16)
        sums.append(dot(c_blk if back else b_blk, sent, 0, 0))
        carries.append(carry_x)
        scores = dot(c_blk, b_blk, 1, 1)
        column = dot(split3(cum), tall, 0, 0)
        for pair in range(8):
            lanes = slice(128 * pair, 128 * pair + 128)
            mixes = []
            for h in (2 * pair, 2 * pair + 1):
                gap = column[:, 128 * h : 128 * h + 128] - cum[h : h + 1, :]
                decays = jnp.exp(jnp.where(mask, gap, -1e30))
                mixes.append((decays * dt_blk[h : h + 1, :] * scores).astype(BF16))
            xp = x_ref[sl, lanes]
            zero = jnp.zeros_like(xp)
            x2 = jnp.concatenate([jnp.where(left_half, xp, zero), jnp.where(left_half, zero, xp)], axis=0)
            if back:
                inside = dot(jnp.concatenate(mixes, axis=0), x2, 0, 0)
            else:
                inside = dot(jnp.concatenate(mixes, axis=1), x2, 1, 0)
            base[sl, lanes] = inside + skip_x[:, lanes] * xp.astype(F32)
    early, late = (1, 0) if back else (0, 1)
    inner[...] = sums[early]
    carry_row[...] = carries[early]
    total = carries[late][0:1] * sums[early] + sums[late]
    both_decay = carries[0][0:1] * carries[1][0:1]
    for lg in range(4):
        decay[lg] = both_decay[:, 256 * lg : 256 * lg + 256]
        for ng in range(8):
            pieces[ng * 4 + lg] = total[16 * ng : 16 * ng + 16, 256 * lg : 256 * lg + 256].astype(BF16)


LOCAL_OUTS = (
    jax.ShapeDtypeStruct((NSLAB, 16, 256), BF16),
    jax.ShapeDtypeStruct((4, 1, 256), F32),
    jax.ShapeDtypeStruct((TOKENS, WIDE), F32),
    jax.ShapeDtypeStruct((HEADS, TOKENS), F32),
    jax.ShapeDtypeStruct((SPAN, WIDE), F32),
    jax.ShapeDtypeStruct((8, WIDE), F32),
)


def bounds_of(lengths):
    b1 = lengths[0]
    b2 = b1 + lengths[1]
    return (b1, b2, b2 + lengths[2])


def back_local_kernel(seg, bc_ref, dt_ref, g_ref, rate_ref, skip_ref, pdt_ref, *rest):
    outs, bvec_out, pdt_out = rest[:6], rest[6], rest[7]
    scratch, dt_pad = rest[8], rest[9]
    z, xl, c, xh, y = place()
    first = (z * 4 + xl * 2 + c) * TOKENS
    heads_first = (xh * 4 + y) * HEADS
    group = xh * 2 + y // 2
    lanes = iota((32, 128), 1)
    taps = pdt_ref[...].astype(F32)
    for g in range(4):
        turned = pltpu.roll(taps, lax.rem(32 * (y - g) + 128, 128), 1)
        mine = jnp.where((lanes >> 5) == y, turned, 0.0).astype(BF16)
        pdt_out[g, :, 0:128] = mine[0:16]
        pdt_out[g, :, 128:256] = mine[16:32]
    b_lanes = pl.ds(pl.multiple_of(group * 128, 128), 128)
    c_lanes = pl.ds(pl.multiple_of(group * 128 + 512, 128), 128)
    bvec_out[...] = bc_ref[:, b_lanes]
    dt_pad[...] = jnp.zeros_like(dt_pad)
    dt_pad[:, 0:HEADS] = dt_ref[...]
    dt = dt_pad[...].T[0:HEADS, :]
    rate = per_head_column(rate_ref[...], scratch, heads_first)
    skip = per_head_column(skip_ref[...], scratch, heads_first)
    local_math(
        True,
        lambda k: bc_ref[pl.ds(SPAN * k, SPAN), b_lanes],
        lambda k: bc_ref[pl.ds(SPAN * k, SPAN), c_lanes],
        dt, rate, skip, g_ref, bounds_of(seg), first, outs,
    )


def next_local_kernel(seg, bc_ref, dt_ref, x_ref, rate_ref, skip_ref, bias_ref, *rest):
    outs, scratch = rest[:6], rest[6]
    z, xl, c, xh, y = place()
    first = (z * 4 + xl * 2 + c) * TOKENS
    heads_first = (xh * 4 + y) * HEADS
    bias = per_head_column(bias_ref[...], scratch, heads_first)[:, 0:1]
    v = dt_ref[...] + bias
    dt = jnp.maximum(v, 0.0) + jnp.log1p(jnp.exp(-jnp.abs(v)))
    rate = per_head_column(rate_ref[...], scratch, heads_first)
    skip = per_head_column(skip_ref[...], scratch, heads_first)
    local_math(
        False,
        lambda k: bc_ref[pl.ds(SPAN * k, SPAN), 0:128],
        lambda k: bc_ref[pl.ds(SPAN * k, SPAN), 128:256],
        dt, rate, skip, x_ref, bounds_of(seg), first, outs,
    )


def final_math(back, pieces, base, factor, inner, carry_row, vec, out):
    first, second = (1, 0) if back else (0, 1)
    wide = spread_matrix(6)
    fl = slice(SPAN * first, SPAN * first + SPAN)
    sl = slice(SPAN * second, SPAN * second + SPAN)
    fac_f = dot(split3(factor[:, fl]), wide, 0, 0)
    fac_s = dot(split3(factor[:, sl]), wide, 0, 0)
    vec_f, vec_s = vec[fl, :], vec[sl, :]
    for lg in range(4):
        lanes = slice(256 * lg, 256 * lg + 256)
        state = jnp.concatenate([pieces[ng * 4 + lg] for ng in range(8)], axis=0)
        read_f = dot(vec_f, state, 1, 0)
        later = carry_row[0:1, lanes] * state.astype(F32) + inner[:, lanes]
        hi = later.astype(BF16)
        low = (later - hi.astype(F32)).astype(BF16)
        read_s = dot(vec_s, hi, 1, 0) + dot(vec_s, low, 1, 0)
        out[fl, lanes] = (base[fl, lanes] + fac_f[:, lanes] * read_f).astype(BF16)
        out[sl, lanes] = (base[sl, lanes] + fac_s[:, lanes] * read_s).astype(BF16)


def final_kernel(*refs):
    n_pieces, n_base, n_factor, n_inner, n_carry, bc = refs[:6]
    b_pieces, b_base, b_factor, b_inner, b_carry, bvec = refs[6:12]
    out_next, out_back = refs[12:14]
    final_math(False, n_pieces, n_base, n_factor, n_inner, n_carry, bc.at[:, 128:256], out_next)
    final_math(True, b_pieces, b_base, b_factor, b_inner, b_carry, bvec, out_back)


def slab_id(index):
    return {"z": index // 4, "xl": lax.rem(index // 2, 2), "c": lax.rem(index, 2)}


class Scan:
    def __init__(self, me, pieces, decay, inbox, decay_in, outbox, landed, sems):
        self.me, self.pieces, self.decay = me, pieces, decay
        self.inbox, self.decay_in, self.outbox, self.landed = inbox, decay_in, outbox, landed
        self.sems = sems

    def piece_copy(self, target, source):
        s, r = self.sems[0], self.sems[1]
        return pltpu.make_async_remote_copy(
            self.pieces.at[target], self.inbox.at[source], s.at[target], r.at[source],
            device_id=slab_id(target), device_id_type=MESH)

    def decay_copy(self, target, source):
        s, r = self.sems[2], self.sems[3]
        return pltpu.make_async_remote_copy(
            self.decay.at[lax.rem(target, 4)], self.decay_in.at[source], s.at[target], r.at[source],
            device_id=slab_id(target), device_id_type=MESH)

    def state_copy(self, target, source):
        s, r = self.sems[4], self.sems[5]
        return pltpu.make_async_remote_copy(
            self.outbox.at[target], self.landed.at[source], s.at[target], r.at[source],
            device_id=slab_id(target), device_id_type=MESH)

    def others(self, body):
        def step(d, carry):
            body(lax.rem(self.me + d, NSLAB))
            return carry

        lax.fori_loop(1, NSLAB, step, 0)

    def send_pieces(self):
        def go(j):
            self.piece_copy(j, self.me).start()
            self.decay_copy(j, self.me).start()

        self.others(go)
        self.inbox[self.me] = self.pieces[self.me]
        self.decay_in[self.me] = self.decay[lax.rem(self.me, 4)]

    def prefix(self, back):
        def arrive(j):
            self.piece_copy(j, j).wait_recv()
            self.decay_copy(j, j).wait_recv()

        self.others(arrive)

        def step(k, state):
            j = NSLAB - 1 - k if back else k
            self.outbox[j] = state.astype(BF16)
            return self.decay_in[j] * state + self.inbox[j].astype(F32)

        lax.fori_loop(0, NSLAB, step, jnp.zeros((16, 256), F32))

    def send_states(self):
        self.others(lambda j: self.state_copy(j, self.me).start())
        self.landed[self.me] = self.outbox[self.me]

    def finish(self):
        def done(j):
            self.state_copy(j, j).wait_recv()
            self.piece_copy(j, self.me).wait_send()
            self.decay_copy(j, self.me).wait_send()
            self.state_copy(j, self.me).wait_send()

        self.others(done)


SCAN_SCRATCH = [
    pltpu.VMEM((NSLAB, 16, 256), BF16),
    pltpu.VMEM((NSLAB, 1, 256), F32),
    pltpu.VMEM((NSLAB, 16, 256), BF16),
    pltpu.VMEM((NSLAB, 16, 256), BF16),
] + [pltpu.SemaphoreType.DMA((NSLAB,))] * 6


def next_scan_kernel(pieces, decay, out, inbox, decay_in, outbox, landed, *sems):
    z, xl, c, xh, y = place()
    me = z * 4 + xl * 2 + c
    scan = Scan(me, pieces, decay, inbox, decay_in, outbox, landed, sems)
    barrier = pltpu.get_barrier_semaphore()
    scan.others(lambda j: pl.semaphore_signal(barrier, inc=1, device_id=slab_id(j), device_id_type=MESH))
    pl.semaphore_wait(barrier, NSLAB - 1)
    scan.send_pieces()
    scan.prefix(False)
    scan.send_states()
    scan.finish()
    out[...] = landed[...]


def project_kernel(hid, pbc, pdt, pieces, decay, bc_out, dt_out, state_out,
                   wbuf, ptmp, hbuf, acc, dts, bc_send, bc_recv, dt_recv,
                   hid_sem, a2a_send, a2a_recv, ring_send, ring_recv, pair_send, pair_recv,
                   inbox, decay_in, outbox, landed, *sems):
    z, xl, c, xh, y = place()
    me = z * 4 + xl * 2 + c
    half = lax.rem(y, 2)
    y_pair = y + 1 - 2 * half
    scan = Scan(me, pieces, decay, inbox, decay_in, outbox, landed, sems)

    barrier = pltpu.get_barrier_semaphore()

    def greet(**where):
        pl.semaphore_signal(barrier, inc=1, device_id=where, device_id_type=MESH)

    scan.others(lambda j: greet(**slab_id(j)))
    greet(y=y_pair)
    own_in_group = xh == half
    for src in range(4):
        @pl.when(jnp.logical_not(own_in_group & (y == src)))
        def _():
            greet(xh=half, y=jnp.int32(src))

    hid_copies = []
    for j in range(NSLAB):
        lanes = pl.ds(pl.multiple_of(256 * j + 128 * half, 128), 128)
        copy = pltpu.make_async_copy(hid.at[:, lanes], hbuf.at[:, pl.ds(128 * j, 128)], hid_sem.at[j])
        copy.start()
        hid_copies.append(copy)

    @pl.when(own_in_group)
    def _():
        pl.semaphore_wait(barrier, NSLAB - 1 + 1 + 3)

    @pl.when(jnp.logical_not(own_in_group))
    def _():
        pl.semaphore_wait(barrier, NSLAB - 1 + 1 + 4)

    my_rows = pl.ds(pl.multiple_of(32 * y, 32), 32)

    def spread_copies(g, source, where):
        rows = pl.ds(pl.multiple_of(32 * source, 32), 32)
        return [
            pltpu.make_async_remote_copy(
                pbc.at[:, pl.ds(128 * g, 128)], wbuf.at[me, rows, pl.ds(0, 128)],
                a2a_send.at[g, 0], a2a_recv.at[source, 0], device_id=where, device_id_type=MESH),
            pltpu.make_async_remote_copy(
                pbc.at[:, pl.ds(512 + 128 * g, 128)], wbuf.at[me, rows, pl.ds(128, 128)],
                a2a_send.at[g, 1], a2a_recv.at[source, 1], device_id=where, device_id_type=MESH),
            pltpu.make_async_remote_copy(
                pdt.at[g], ptmp.at[source],
                a2a_send.at[g, 2], a2a_recv.at[source, 2], device_id=where, device_id_type=MESH),
        ]

    for g in range(4):
        to_y = 2 * (g % 2) + xh
        mine = (xh == g // 2) & (y == to_y)
        where = {"xh": jnp.int32(g // 2), "y": to_y}

        @pl.when(jnp.logical_not(mine))
        def _():
            for copy in spread_copies(g, y, where):
                copy.start()

        @pl.when(mine)
        def _():
            wbuf[me, my_rows, 0:128] = pbc[:, 128 * g : 128 * g + 128]
            wbuf[me, my_rows, 128:256] = pbc[:, 512 + 128 * g : 512 + 128 * g + 128]
            ptmp[y] = pdt[g]

    scan.send_pieces()

    for src in range(4):
        @pl.when(jnp.logical_not(own_in_group & (y == src)))
        def _():
            for copy in spread_copies(0, src, {"xh": half, "y": jnp.int32(src)}):
                copy.wait_recv()

    packed = (ptmp[0].astype(F32) + ptmp[1].astype(F32)) + (ptmp[2].astype(F32) + ptmp[3].astype(F32))
    wbuf[me, 128:144, :] = packed.astype(BF16)

    right, left = lax.rem(z + 1, NZ), lax.rem(z + NZ - 1, NZ)
    ROWS = (pl.ds(0, 64), pl.ds(64, 80))
    sends = []

    def forward(slot, chunk, **where):
        part = wbuf.at[slot, ROWS[chunk]]
        copy = pltpu.make_async_remote_copy(
            part, part, ring_send.at[len(sends)], ring_recv.at[slot, chunk],
            device_id=where, device_id_type=MESH)
        copy.start()
        sends.append(copy)

    def arrive(slot, chunk):
        part = wbuf.at[slot, ROWS[chunk]]
        pltpu.make_async_remote_copy(
            part, part, ring_send.at[0], ring_recv.at[slot, chunk],
            device_id={"z": right}, device_id_type=MESH).wait_recv()

    mate = me + 2 - 4 * xl
    sibling = me + 1 - 2 * c
    other_x, other_c = 1 - xl, 1 - c
    for chunk in (0, 1):
        forward(me, chunk, xl=other_x)
        forward(me, chunk, z=right)
        forward(me, chunk, z=left)
    for chunk in (0, 1):
        forward(me, chunk, c=other_c)
    arrive(mate, 0)
    forward(mate, 0, z=right)
    forward(mate, 0, z=left)
    forward(mate, 0, c=other_c)
    last = {0: (1,), 1: (0, 2)}
    late = [mate]
    for hop in range(1, 5):
        fresh = []
        for chunk in (0, 1, 2):
            for side in (0, 1):
                if hop == 4 and chunk not in last[side]:
                    continue
                oz = lax.rem(z + NZ - hop, NZ) if side == 0 else lax.rem(z + hop, NZ)
                column = oz * 4 + xl * 2 + c
                across = oz * 4 + other_x * 2 + c
                slot, part = (across, 0) if chunk == 2 else (column, chunk)
                arrive(slot, part)
                if hop < 3 or (hop == 3 and chunk in last[side]):
                    forward(slot, part, z=right if side == 0 else left)
                if chunk == 1:
                    forward(slot, 1, xl=other_x)
                    fresh.append(across)
                forward(slot, part, c=other_c)
        for slot in late:
            arrive(slot, 1)
            forward(slot, 1, c=other_c)
        late = fresh
    for slot in late:
        arrive(slot, 1)
        forward(slot, 1, c=other_c)

    scan.prefix(True)
    scan.send_states()

    for copy in hid_copies:
        copy.wait()
    for oz in range(NZ):
        for ox in range(2):
            for chunk in (0, 1):
                arrive(oz * 4 + ox * 2 + other_c, chunk)

    acc[...] = jnp.zeros_like(acc)
    lane_class = iota((32, 128), 1) >> 5

    def multiply(j, carry):
        columns = hbuf[:, pl.ds(pl.multiple_of(256 * j, 256), 256)]
        weights, taps = [], []
        for k in (2 * j, 2 * j + 1):
            weights.append(wbuf[k, 0:128, :])
            low = wbuf[k, 128:144, :].astype(F32)
            block = jnp.concatenate([low[:, 0:128], low[:, 128:256]], axis=0)
            taps += [jnp.where(lane_class == i, block, 0.0) for i in range(4)]
        acc[:, 0:256] += dot(columns, jnp.concatenate(weights, axis=0), 1, 0)
        acc[:, 256:384] += dot(columns, jnp.concatenate(taps, axis=0).astype(BF16), 1, 0)
        return carry

    lax.fori_loop(0, 16, multiply, 0)

    folded = acc[:, 256:384].T
    dts[...] = (folded[0:32] + folded[32:64]) + (folded[64:96] + folded[96:128])
    bc_send[...] = acc[:, 0:256].astype(BF16)
    pair = [
        pltpu.make_async_remote_copy(
            bc_send, bc_recv, pair_send.at[0], pair_recv.at[0],
            device_id={"y": y_pair}, device_id_type=MESH),
        pltpu.make_async_remote_copy(
            dts.at[pl.ds(pl.multiple_of(16 - 16 * half, 16), 16)], dt_recv, pair_send.at[1], pair_recv.at[1],
            device_id={"y": y_pair}, device_id_type=MESH),
    ]
    for copy in pair:
        copy.start()
    for copy in pair:
        copy.wait_recv()
    bc_out[...] = (acc[:, 0:256] + bc_recv[...].astype(F32)).astype(BF16)
    dt_out[...] = dts[pl.ds(pl.multiple_of(16 * half, 16), 16)] + dt_recv[...]

    for g in range(4):
        to_y = 2 * (g % 2) + xh
        mine = (xh == g // 2) & (y == to_y)

        @pl.when(jnp.logical_not(mine))
        def _():
            for copy in spread_copies(g, y, {"xh": jnp.int32(g // 2), "y": to_y}):
                copy.wait_send()

    for copy in sends:
        copy.wait_send()
    for copy in pair:
        copy.wait_send()
    scan.finish()
    state_out[...] = landed[...]


def params(limit_mib, **kw):
    return pltpu.CompilerParams(vmem_limit_bytes=limit_mib << 20, **kw)


def body(hidden_next, values_next, seg_next, proj_bc, proj_dt, dt_bias, decay_rate, skip_gain,
         bc_prev, dt_prev, seg_prev, grad_prev):
    as_row = lambda a: a.reshape(1, 128)
    bias, rate, skip = as_row(dt_bias), as_row(decay_rate), as_row(skip_gain)
    sds = jax.ShapeDtypeStruct
    *back, bvec, pdt = pl.pallas_call(
        back_local_kernel,
        out_shape=LOCAL_OUTS + (sds((TOKENS, 128), BF16), sds((4, 16, 256), BF16)),
        in_specs=[SMEM] + [VMEM] * 6,
        out_specs=(VMEM,) * 8,
        scratch_shapes=[pltpu.VMEM((128, 128), F32), pltpu.VMEM((TOKENS, 128), F32)],
        compiler_params=params(40),
        name="back_local",
    )(seg_prev, bc_prev, dt_prev, grad_prev, rate, skip, proj_dt)
    bc, dt_pre, back_states = pl.pallas_call(
        project_kernel,
        out_shape=(sds((TOKENS, 256), BF16), sds((HEADS, TOKENS), F32), sds((NSLAB, 16, 256), BF16)),
        in_specs=[ANY] + [VMEM] * 4,
        out_specs=(VMEM,) * 3,
        scratch_shapes=[
            pltpu.VMEM((NSLAB, 144, 256), BF16),
            pltpu.VMEM((4, 16, 256), BF16),
            pltpu.VMEM((TOKENS, 4096), BF16),
            pltpu.VMEM((TOKENS, 384), F32),
            pltpu.VMEM((32, TOKENS), F32),
            pltpu.VMEM((TOKENS, 256), BF16),
            pltpu.VMEM((TOKENS, 256), BF16),
            pltpu.VMEM((HEADS, TOKENS), F32),
            pltpu.SemaphoreType.DMA((NSLAB,)),
            pltpu.SemaphoreType.DMA((4, 3)),
            pltpu.SemaphoreType.DMA((4, 3)),
            pltpu.SemaphoreType.DMA((80,)),
            pltpu.SemaphoreType.DMA((NSLAB, 2)),
            pltpu.SemaphoreType.DMA((2,)),
            pltpu.SemaphoreType.DMA((2,)),
        ] + SCAN_SCRATCH,
        compiler_params=params(40, collective_id=0, has_side_effects=True),
        name="project",
    )(hidden_next, proj_bc, pdt, back[0], back[1])
    nxt = pl.pallas_call(
        next_local_kernel,
        out_shape=LOCAL_OUTS,
        in_specs=[SMEM] + [VMEM] * 6,
        out_specs=(VMEM,) * 6,
        scratch_shapes=[pltpu.VMEM((128, 128), F32)],
        compiler_params=params(40),
        name="next_local",
    )(seg_next, bc, dt_pre, values_next, rate, skip, bias)
    next_states = pl.pallas_call(
        next_scan_kernel,
        out_shape=sds((NSLAB, 16, 256), BF16),
        in_specs=[VMEM] * 2,
        out_specs=VMEM,
        scratch_shapes=SCAN_SCRATCH,
        compiler_params=params(16, collective_id=1, has_side_effects=True),
        name="next_scan",
    )(nxt[0], nxt[1])
    return pl.pallas_call(
        final_kernel,
        out_shape=(sds((TOKENS, WIDE), BF16), sds((TOKENS, WIDE), BF16)),
        in_specs=[VMEM] * 12,
        out_specs=(VMEM,) * 2,
        compiler_params=params(40),
        name="final",
    )(next_states, *nxt[2:], bc, back_states, *back[2:], bvec)


def solution(mesh):
    split = Mesh(mesh.devices.reshape(8, 2, 2, 2, 4), ("z", "xl", "c", "xh", "y"))
    tokens, both, rows = P(SEQ, None), P(SEQ, FSDP), P(SEQ + FSDP, None)
    in_specs = (tokens, both, P(), rows, rows, P(), P(), P(), tokens, both, P(), both)
    return jax.shard_map(body, mesh=split, in_specs=in_specs, out_specs=(both, both), check_vma=False)
```

```python
import functools

import jax
import jax.numpy as jnp
from jax import lax
from jax.experimental import pallas as pl
from jax.experimental.pallas import tpu as pltpu
from jax.sharding import Mesh
from jax.sharding import PartitionSpec as P

MESH = pl.DeviceIdType.MESH
SEQ = ("z", "xl", "c")
FSDP = ("xh", "y")
F32, BF16, I32 = jnp.float32, jnp.bfloat16, jnp.int32
NZ, NSLAB = 8, 32
SPAN, HEADS, WIDE = 128, 16, 1024
TOKENS = 256
VMEM = pl.BlockSpec(memory_space=pltpu.VMEM)
SMEM = pl.BlockSpec(memory_space=pltpu.SMEM)
ANY = pl.BlockSpec(memory_space=pl.ANY)


def iota(shape, dim):
    return lax.broadcasted_iota(I32, shape, dim)


def place():
    z, xl, c = lax.axis_index("z"), lax.axis_index("xl"), lax.axis_index("c")
    xh, y = lax.axis_index("xh"), lax.axis_index("y")
    return z, xl, c, xh, y


def dot(a, b, ca, cb):
    return lax.dot_general(a, b, (((ca,), (cb,)), ((), ())), preferred_element_type=F32)


def split3(v):
    hi = v.astype(BF16)
    rest = v - hi.astype(F32)
    mid = rest.astype(BF16)
    low = (rest - mid.astype(F32)).astype(BF16)
    return jnp.concatenate([hi, mid, low], axis=0)


def spread_matrix(shift):
    n = HEADS << shift
    same = (iota((48, n), 0) & 15) == (iota((48, n), 1) >> shift)
    return jnp.where(same, 1.0, 0.0).astype(BF16)


def per_head_column(row, scratch, first_head):
    scratch[...] = jnp.broadcast_to(row, (128, 128)).T
    return scratch[pl.ds(pl.multiple_of(first_head, HEADS), HEADS), :]


def segment_of(bounds, places):
    count = [jnp.where(places >= b, 1, 0).astype(I32) for b in bounds]
    return count[0] + count[1] + count[2]


def scalar_segment(bounds, position):
    count = [(position >= b).astype(I32) for b in bounds]
    return count[0] + count[1] + count[2]


def bounds_of(lengths):
    b1 = lengths[0]
    b2 = b1 + lengths[1]
    return (b1, b2, b2 + lengths[2])


class Side:
    def __init__(self, back, refs, first, bounds, rate, skip):
        (self.bv, self.cv, self.values, self.dt, self.cum, self.factor, self.base, self.inner, self.carry_row,
         self.total, self.decay) = refs
        self.back, self.first, self.bounds, self.rate, self.skip = back, first, bounds, rate, skip

    def summarize(self):
        wide = spread_matrix(6)
        rows, cols = iota((SPAN, SPAN), 0), iota((SPAN, SPAN), 1)
        upper = jnp.where(rows <= cols, 1.0, 0.0).astype(BF16)
        back, bounds = self.back, self.bounds
        sums, carries = [], []
        for blk in range(2):
            sl = slice(SPAN * blk, SPAN * blk + SPAN)
            dt = self.dt[:, sl]
            parts = dot(split3(-(dt * self.rate[...])), upper, 1, 0)
            cum = parts[0:16] + (parts[16:32] + parts[32:48])
            self.cum[:, sl] = cum
            start = self.first + SPAN * blk
            seg_end = scalar_segment(bounds, start + (SPAN - 1))
            seg_before = scalar_segment(bounds, start - 1)
            seg_row = segment_of(bounds, start + iota((HEADS, SPAN), 1))
            cum_end = jnp.broadcast_to(cum[:, SPAN - 1 : SPAN], (HEADS, SPAN))
            send = jnp.where(seg_row == seg_end, jnp.exp(cum_end - cum) * dt, 0.0)
            read = jnp.where(seg_row == seg_before, jnp.exp(cum), 0.0)
            carry = jnp.exp(cum_end) * jnp.where(seg_end == seg_before, 1.0, 0.0)
            carries.append(dot(split3(carry), wide, 0, 0)[0:8])
            self.factor[:, sl] = send if back else read
            scale = dot(split3(read if back else send), wide, 0, 0)
            sent = (self.values[sl, :].astype(F32) * scale).astype(BF16)
            sums.append(dot((self.cv if back else self.bv)[sl, :], sent, 0, 0))
        early, late = (1, 0) if back else (0, 1)
        self.inner[...] = sums[early]
        self.carry_row[...] = carries[early]
        self.total[...] = carries[late][0:1] * sums[early] + sums[late]
        self.decay[...] = carries[0] * carries[1]

    def within(self):
        tall = spread_matrix(7)
        wide = spread_matrix(6)
        rows, cols = iota((SPAN, SPAN), 0), iota((SPAN, SPAN), 1)
        left_half = cols < 64
        back, bounds = self.back, self.bounds
        skip_x = dot(split3(self.skip[...]), wide, 0, 0)[0:1]

        def block(blk, carry):
            sl = pl.ds(pl.multiple_of(SPAN * blk, SPAN), SPAN)
            cum, dt = self.cum[:, sl], self.dt[:, sl]
            start = self.first + SPAN * blk
            mask = (segment_of(bounds, start + rows) == segment_of(bounds, start + cols)) & (rows >= cols)
            scores = dot(self.cv[sl, :], self.bv[sl, :], 1, 1)
            column = dot(split3(cum), tall, 0, 0)
            for pair in range(8):
                lanes = slice(128 * pair, 128 * pair + 128)
                mixes = []
                for h in (2 * pair, 2 * pair + 1):
                    gap = column[:, 128 * h : 128 * h + 128] - cum[h : h + 1, :]
                    decays = jnp.exp(jnp.where(mask, gap, -1e30))
                    mixes.append((decays * dt[h : h + 1, :] * scores).astype(BF16))
                xp = self.values[sl, lanes]
                zero = jnp.zeros_like(xp)
                x2 = jnp.concatenate([jnp.where(left_half, xp, zero), jnp.where(left_half, zero, xp)], axis=0)
                if back:
                    inside = dot(jnp.concatenate(mixes, axis=0), x2, 0, 0)
                else:
                    inside = dot(jnp.concatenate(mixes, axis=1), x2, 1, 0)
                self.base[sl, lanes] = inside + skip_x[:, lanes] * xp.astype(F32)
            return carry

        lax.fori_loop(0, 2, block, 0)

    def finish(self, state, out):
        wide = spread_matrix(6)
        first, second = (1, 0) if self.back else (0, 1)
        vec = self.bv if self.back else self.cv
        for blk, later in ((first, False), (second, True)):
            sl = slice(SPAN * blk, SPAN * blk + SPAN)
            scale = dot(split3(self.factor[:, sl]), wide, 0, 0)
            for half in range(2):
                lanes = slice(512 * half, 512 * half + 512)
                now = state[half]
                if later:
                    now = self.carry_row[0:1, lanes] * now + self.inner[:, lanes]
                hi = now.astype(BF16)
                low = (now - hi.astype(F32)).astype(BF16)
                read = dot(vec[sl, :], hi, 1, 0) + dot(vec[sl, :], low, 1, 0)
                out[sl, lanes] = (self.base[sl, lanes] + scale[:, lanes] * read).astype(BF16)


NCHIP = 16


def chip_id(q):
    return {"z": q // 2, "xl": lax.rem(q, 2)}


class Scan:
    def __init__(self, back, me, core, total, decay, refs):
        self.back, self.me, self.core, self.total, self.decay = back, me, core, total, decay
        (self.sib_total, self.sib_decay, self.pieces, self.steps, self.inbox, self.decay_in, self.outbox, self.landed,
         self.away, self.state) = refs[:10]
        self.sems = refs[10:]

    def to_chip(self, src, dst, k, target, source):
        return pltpu.make_async_remote_copy(
            src, dst, self.sems[k].at[target], self.sems[k + 1].at[source],
            device_id=chip_id(target), device_id_type=MESH)

    def piece_copy(self, target, source):
        return self.to_chip(self.pieces.at[target], self.inbox.at[source], 0, target, source)

    def decay_copy(self, target, source):
        return self.to_chip(self.steps.at[lax.rem(target, 2)], self.decay_in.at[source], 2, target, source)

    def state_copy(self, target, source):
        return self.to_chip(self.outbox.at[target], self.landed.at[source], 4, target, source)

    def to_sibling(self, src, dst, k):
        return pltpu.make_async_remote_copy(
            src, dst, self.sems[6].at[k], self.sems[7].at[k],
            device_id={"c": 1 - self.core}, device_id_type=MESH)

    def lanes(self, core):
        return pl.ds(pl.multiple_of(512 * core, 512), 512)

    def sibling_copies(self):
        theirs = self.lanes(1 - self.core)
        return (self.to_sibling(self.total.at[:, theirs], self.sib_total, 0),
                self.to_sibling(self.decay.at[:, theirs], self.sib_decay, 1))

    def back_copy(self):
        return self.to_sibling(self.away, self.state.at[self.core], 2)

    def others(self, body):
        def step(d, carry):
            body(lax.rem(self.me + d, NCHIP))
            return carry

        lax.fori_loop(1, NCHIP, step, 0)

    def share(self):
        for copy in self.sibling_copies():
            copy.start()

    def two_slabs(self):
        mine = self.lanes(self.core)
        own, own_decay = self.total[:, mine], self.decay[0:1, mine]
        sib, sib_decay = self.sib_total[...], self.sib_decay[0:1]
        own_first = self.core == (1 if self.back else 0)
        pick = lambda a, b: (jnp.where(own_first, a, b), jnp.where(own_first, b, a))
        return own_first, pick(own, sib), pick(own_decay, sib_decay)

    def join(self):
        for copy in self.sibling_copies():
            copy.wait_recv()
        _, (sum0, sum1), (decay0, decay1) = self.two_slabs()
        chip = decay1 * sum0 + sum1
        chip_decay = decay0 * decay1
        for lg in range(2):
            self.steps[lg] = chip_decay[:, 256 * lg : 256 * lg + 256]
            for ng in range(8):
                self.pieces[ng * 2 + lg] = chip[16 * ng : 16 * ng + 16, 256 * lg : 256 * lg + 256].astype(BF16)

    def send_pieces(self):
        def go(q):
            self.piece_copy(q, self.me).start()
            self.decay_copy(q, self.me).start()

        self.others(go)
        self.inbox[self.me] = self.pieces[self.me]
        self.decay_in[self.me] = self.steps[lax.rem(self.me, 2)]

    def prefix(self):
        def arrive(q):
            self.piece_copy(q, q).wait_recv()
            self.decay_copy(q, q).wait_recv()

        self.others(arrive)

        def step(k, state):
            q = NCHIP - 1 - k if self.back else k
            self.outbox[q] = state.astype(BF16)
            return self.decay_in[q] * state + self.inbox[q].astype(F32)

        lax.fori_loop(0, NCHIP, step, jnp.zeros((16, 256), F32))

    def send_states(self):
        self.others(lambda q: self.state_copy(q, self.me).start())
        self.landed[self.me] = self.outbox[self.me]

    def collect(self):
        self.others(lambda q: self.state_copy(q, q).wait_recv())
        own_first, (sum0, _), (decay0, _) = self.two_slabs()
        chip = jnp.concatenate(
            [jnp.concatenate([self.landed[2 * ng], self.landed[2 * ng + 1]], axis=1) for ng in range(8)], axis=0
        ).astype(F32)
        then = decay0 * chip + sum0
        self.state[self.core] = jnp.where(own_first, chip, then)
        self.away[...] = jnp.where(own_first, then, chip)
        self.back_copy().start()

    def ready(self):
        self.back_copy().wait_recv()

    def drain(self):
        def done(q):
            self.piece_copy(q, self.me).wait_send()
            self.decay_copy(q, self.me).wait_send()
            self.state_copy(q, self.me).wait_send()

        self.others(done)
        for copy in self.sibling_copies():
            copy.wait_send()
        self.back_copy().wait_send()


def scan_scratch():
    return [
        pltpu.VMEM((SPAN, 512), F32),
        pltpu.VMEM((8, 512), F32),
        pltpu.VMEM((NCHIP, 16, 256), BF16),
        pltpu.VMEM((2, 1, 256), F32),
        pltpu.VMEM((NCHIP, 16, 256), BF16),
        pltpu.VMEM((NCHIP, 1, 256), F32),
        pltpu.VMEM((NCHIP, 16, 256), BF16),
        pltpu.VMEM((NCHIP, 16, 256), BF16),
        pltpu.VMEM((SPAN, 512), F32),
        pltpu.VMEM((2, SPAN, 512), F32),
    ] + [pltpu.SemaphoreType.DMA((NCHIP,))] * 6 + [pltpu.SemaphoreType.DMA((3,))] * 2


def side_scratch():
    return [
        pltpu.VMEM((TOKENS, 128), BF16),
        pltpu.VMEM((TOKENS, 128), BF16),
        pltpu.VMEM((TOKENS, WIDE), BF16),
        pltpu.VMEM((HEADS, TOKENS), F32),
        pltpu.VMEM((HEADS, TOKENS), F32),
        pltpu.VMEM((HEADS, TOKENS), F32),
        pltpu.VMEM((TOKENS, WIDE), F32),
        pltpu.VMEM((SPAN, WIDE), F32),
        pltpu.VMEM((8, WIDE), F32),
        pltpu.VMEM((SPAN, WIDE), F32),
        pltpu.VMEM((8, WIDE), F32),
    ]


N_SIDE, N_SCAN = 11, 18
LAST = {0: (1,), 1: (0, 2)}


def kernel(hid, x_in, seg_next, pbc_in, pdt_in, bias_in, rate_in, skip_in, bc_in, dt_in, seg_prev, g_in,
           next_out, back_out, *rest):
    next_refs, rest = rest[:N_SIDE], rest[N_SIDE:]
    back_refs, rest = rest[:N_SIDE], rest[N_SIDE:]
    next_scan_refs, rest = rest[:N_SCAN], rest[N_SCAN:]
    back_scan_refs, rest = rest[:N_SCAN], rest[N_SCAN:]
    (seg_n, seg_p, pbc, taps_in, pdt, bias_row, rate_row, skip_row, column, rate_col, skip_col,
     wbuf, ptmp, hbuf, acc, dts, bc_send, bc_recv, dt_recv, next_res, back_res,
     in_sem, hid_sem, out_sem, a2a_send, a2a_recv, ring_send, ring_recv, pair_send, pair_recv) = rest

    z, xl, c, xh, y = place()
    me = z * 4 + xl * 2 + c
    chip = z * 2 + xl
    half = lax.rem(y, 2)
    y_pair = y + 1 - 2 * half
    group = xh * 2 + y // 2
    heads_first = (xh * 4 + y) * HEADS
    own_in_group = xh == half
    other_x, other_c = 1 - xl, 1 - c
    barrier = pltpu.get_barrier_semaphore()

    def greet(**where):
        pl.semaphore_signal(barrier, inc=1, device_id=where, device_id_type=MESH)

    def meet(d, carry):
        greet(**chip_id(lax.rem(chip + d, NCHIP)))
        return carry

    lax.fori_loop(1, NCHIP, meet, 0)
    greet(c=other_c)
    greet(y=y_pair)
    for src in range(4):
        @pl.when(jnp.logical_not(own_in_group & (y == src)))
        def _():
            greet(xh=half, y=jnp.int32(src))

    b_lanes = pl.ds(pl.multiple_of(group * 128, 128), 128)
    c_lanes = pl.ds(pl.multiple_of(group * 128 + 512, 128), 128)
    loads = {}
    for k, (name, src, dst) in enumerate((
        ("taps", pdt_in, taps_in), ("pbc", pbc_in, pbc),
        ("rate", rate_in, rate_row), ("skip", skip_in, skip_row), ("bias", bias_in, bias_row),
        ("seg_p", seg_prev, seg_p), ("seg_n", seg_next, seg_n),
        ("dt", dt_in, back_refs[3]), ("b", bc_in.at[:, b_lanes], back_refs[0]), ("c", bc_in.at[:, c_lanes], back_refs[1]),
        ("g", g_in, back_refs[2]), ("x", x_in, next_refs[2]),
    )):
        loads[name] = pltpu.make_async_copy(src, dst, in_sem.at[k])
        loads[name].start()

    def hid_copy(j):
        lanes = pl.ds(pl.multiple_of(256 * j + 128 * half, 128), 128)
        return pltpu.make_async_copy(
            hid.at[:, lanes], hbuf.at[:, pl.ds(pl.multiple_of(128 * j, 128), 128)], hid_sem.at[j])

    def load_hid(j, carry):
        hid_copy(j).start()
        return carry

    lax.fori_loop(0, NSLAB, load_hid, 0)

    loads["taps"].wait()
    lane_class = iota((32, 128), 1) >> 5
    taps = taps_in[...].astype(F32)
    for g in range(4):
        turned = pltpu.roll(taps, lax.rem(32 * (y - g) + 128, 128), 1)
        mine = jnp.where(lane_class == y, turned, 0.0).astype(BF16)
        pdt[g, :, 0:128] = mine[0:16]
        pdt[g, :, 128:256] = mine[16:32]
    for name in ("rate", "skip", "bias", "seg_p", "seg_n", "pbc"):
        loads[name].wait()
    rate_col[...] = per_head_column(rate_row[...], column, heads_first)
    skip_col[...] = per_head_column(skip_row[...], column, heads_first)
    bias_col = per_head_column(bias_row[...], column, heads_first)[:, 0:1]
    nxt = Side(False, next_refs, me * TOKENS, bounds_of(seg_n), rate_col, skip_col)
    back = Side(True, back_refs, me * TOKENS, bounds_of(seg_p), rate_col, skip_col)
    nxt_scan = Scan(False, chip, c, nxt.total, nxt.decay, next_scan_refs)
    back_scan = Scan(True, chip, c, back.total, back.decay, back_scan_refs)


    @pl.when(own_in_group)
    def _():
        pl.semaphore_wait(barrier, NCHIP - 1 + 2 + 3)

    @pl.when(jnp.logical_not(own_in_group))
    def _():
        pl.semaphore_wait(barrier, NCHIP - 1 + 2 + 4)


    my_rows = pl.ds(pl.multiple_of(32 * y, 32), 32)

    def spread_copies(g, source, where):
        rows = pl.ds(pl.multiple_of(32 * source, 32), 32)
        parts = ((pbc.at[:, pl.ds(128 * g, 128)], wbuf.at[me, rows, pl.ds(0, 128)]),
                 (pbc.at[:, pl.ds(512 + 128 * g, 128)], wbuf.at[me, rows, pl.ds(128, 128)]),
                 (pdt.at[g], ptmp.at[source]))
        return [
            pltpu.make_async_remote_copy(
                src, dst, a2a_send.at[g, k], a2a_recv.at[source, k], device_id=where, device_id_type=MESH)
            for k, (src, dst) in enumerate(parts)
        ]

    def spread(g):
        to_y = 2 * (g % 2) + xh
        mine = (xh == g // 2) & (y == to_y)
        return mine, spread_copies(g, y, {"xh": jnp.int32(g // 2), "y": to_y})

    for g in range(4):
        mine, copies = spread(g)

        @pl.when(jnp.logical_not(mine))
        def _():
            for copy in copies:
                copy.start()

        @pl.when(mine)
        def _():
            wbuf[me, my_rows, 0:128] = pbc[:, 128 * g : 128 * g + 128]
            wbuf[me, my_rows, 128:256] = pbc[:, 512 + 128 * g : 512 + 128 * g + 128]
            ptmp[y] = pdt[g]

    for name in ("dt", "b", "c", "g"):
        loads[name].wait()
    back.summarize()
    back_scan.share()

    for src in range(4):
        @pl.when(jnp.logical_not(own_in_group & (y == src)))
        def _():
            for copy in spread_copies(0, src, {"xh": half, "y": jnp.int32(src)}):
                copy.wait_recv()

    packed = (ptmp[0].astype(F32) + ptmp[1].astype(F32)) + (ptmp[2].astype(F32) + ptmp[3].astype(F32))
    wbuf[me, 128:144, :] = packed.astype(BF16)

    right, left = lax.rem(z + 1, NZ), lax.rem(z + NZ - 1, NZ)
    ROWS = (pl.ds(0, 64), pl.ds(64, 80))
    sends = []

    def forward(slot, chunk, **where):
        part = wbuf.at[slot, ROWS[chunk]]
        copy = pltpu.make_async_remote_copy(
            part, part, ring_send.at[len(sends)], ring_recv.at[slot, chunk],
            device_id=where, device_id_type=MESH)
        copy.start()
        sends.append(copy)

    def arrive(slot, chunk):
        part = wbuf.at[slot, ROWS[chunk]]
        pltpu.make_async_remote_copy(
            part, part, ring_send.at[0], ring_recv.at[slot, chunk],
            device_id={"z": right}, device_id_type=MESH).wait_recv()

    def multiply_group(hop):
        def multiply(i, carry):
            if hop in (0, 4):
                oz, ox = lax.rem(z + hop, NZ), i
            else:
                oz, ox = lax.rem(z + NZ - hop + (i // 2) * (2 * hop), NZ), lax.rem(i, 2)
            j = oz * 2 + ox
            for chunk in (0, 1):
                arrive(2 * j + other_c, chunk)
            hid_copy(2 * j).wait()
            hid_copy(2 * j + 1).wait()
            columns = hbuf[:, pl.ds(pl.multiple_of(256 * j, 256), 256)]
            weights, parts = [], []
            for k in (2 * j, 2 * j + 1):
                weights.append(wbuf[k, 0:128, :])
                low = wbuf[k, 128:144, :].astype(F32)
                block = jnp.concatenate([low[:, 0:128], low[:, 128:256]], axis=0)
                parts += [jnp.where(lane_class == q, block, 0.0) for q in range(4)]
            acc[:, 0:256] += dot(columns, jnp.concatenate(weights, axis=0), 1, 0)
            acc[:, 256:384] += dot(columns, jnp.concatenate(parts, axis=0).astype(BF16), 1, 0)
            return carry

        lax.fori_loop(0, 2 if hop in (0, 4) else 4, multiply, 0)

    mate = me + 2 - 4 * xl
    for chunk in (0, 1):
        forward(me, chunk, z=right)
        forward(me, chunk, z=left)
        forward(me, chunk, xl=other_x)
    for chunk in (0, 1):
        forward(me, chunk, c=other_c)
    acc[...] = jnp.zeros_like(acc)
    back.within()
    arrive(mate, 0)
    forward(mate, 0, z=right)
    forward(mate, 0, z=left)
    forward(mate, 0, c=other_c)
    late = [mate]
    for hop in range(1, 5):
        fresh = []
        for chunk in (0, 1, 2):
            for side in (0, 1):
                if hop == 4 and chunk not in LAST[side]:
                    continue
                oz = lax.rem(z + NZ - hop, NZ) if side == 0 else lax.rem(z + hop, NZ)
                column_slot = oz * 4 + xl * 2 + c
                across = oz * 4 + other_x * 2 + c
                slot, part = (across, 0) if chunk == 2 else (column_slot, chunk)
                arrive(slot, part)
                if hop < 3 or (hop == 3 and chunk in LAST[side]):
                    forward(slot, part, z=right if side == 0 else left)
                if chunk == 1:
                    forward(slot, 1, xl=other_x)
                    fresh.append(across)
                forward(slot, part, c=other_c)
        for slot in late:
            arrive(slot, 1)
            forward(slot, 1, c=other_c)
        late = fresh
        if hop == 3:
            back_scan.join()
            back_scan.send_pieces()
        multiply_group(hop - 1)
    for slot in late:
        arrive(slot, 1)
        forward(slot, 1, c=other_c)
    multiply_group(4)

    folded = acc[:, 256:384].T
    dts[...] = (folded[0:32] + folded[32:64]) + (folded[64:96] + folded[96:128])
    bc_send[...] = acc[:, 0:256].astype(BF16)
    their_heads = pl.ds(pl.multiple_of(16 - 16 * half, 16), 16)
    pair = [
        pltpu.make_async_remote_copy(
            src, dst, pair_send.at[k], pair_recv.at[k], device_id={"y": y_pair}, device_id_type=MESH)
        for k, (src, dst) in enumerate(((dts.at[their_heads], dt_recv), (bc_send, bc_recv)))
    ]
    for copy in pair:
        copy.start()
    for copy in pair:
        copy.wait_recv()
    total = acc[:, 0:256] + bc_recv[...].astype(F32)
    nxt.bv[...] = total[:, 0:128].astype(BF16)
    nxt.cv[...] = total[:, 128:256].astype(BF16)
    v = dts[pl.ds(pl.multiple_of(16 * half, 16), 16)] + dt_recv[...] + bias_col
    nxt.dt[...] = jnp.maximum(v, 0.0) + jnp.log1p(jnp.exp(-jnp.abs(v)))
    loads["x"].wait()
    nxt.summarize()
    nxt_scan.share()
    back_scan.prefix()
    nxt_scan.join()
    nxt_scan.send_pieces()
    back_scan.send_states()
    nxt.within()
    nxt_scan.prefix()
    nxt_scan.send_states()
    back_scan.collect()
    back_scan.ready()
    back.finish(back_scan.state, back_res)
    back_write = pltpu.make_async_copy(back_res, back_out, out_sem.at[0])
    back_write.start()
    nxt_scan.collect()
    nxt_scan.ready()
    nxt.finish(nxt_scan.state, next_res)
    next_write = pltpu.make_async_copy(next_res, next_out, out_sem.at[1])
    next_write.start()
    for g in range(4):
        mine, copies = spread(g)

        @pl.when(jnp.logical_not(mine))
        def _():
            for copy in copies:
                copy.wait_send()

    for copy in sends:
        copy.wait_send()
    for copy in pair:
        copy.wait_send()
    back_scan.drain()
    nxt_scan.drain()
    back_write.wait()
    next_write.wait()


def body(hidden_next, values_next, seg_next, proj_bc, proj_dt, dt_bias, decay_rate, skip_gain,
         bc_prev, dt_prev, seg_prev, grad_prev):
    as_row = lambda a: a.reshape(1, 128)
    out = jax.ShapeDtypeStruct((TOKENS, WIDE), BF16)
    dma = pltpu.SemaphoreType.DMA
    return pl.pallas_call(
        kernel,
        out_shape=(out, out),
        in_specs=[ANY] * 12,
        out_specs=(ANY, ANY),
        scratch_shapes=side_scratch() + side_scratch() + scan_scratch() + scan_scratch() + [
            pltpu.SMEM((4,), I32),
            pltpu.SMEM((4,), I32),
            pltpu.VMEM((32, 1024), BF16),
            pltpu.VMEM((32, 128), BF16),
            pltpu.VMEM((4, 16, 256), BF16),
            pltpu.VMEM((1, 128), F32),
            pltpu.VMEM((1, 128), F32),
            pltpu.VMEM((1, 128), F32),
            pltpu.VMEM((128, 128), F32),
            pltpu.VMEM((HEADS, 128), F32),
            pltpu.VMEM((HEADS, 128), F32),
            pltpu.VMEM((NSLAB, 144, 256), BF16),
            pltpu.VMEM((4, 16, 256), BF16),
            pltpu.VMEM((TOKENS, 4096), BF16),
            pltpu.VMEM((TOKENS, 384), F32),
            pltpu.VMEM((32, TOKENS), F32),
            pltpu.VMEM((TOKENS, 256), BF16),
            pltpu.VMEM((TOKENS, 256), BF16),
            pltpu.VMEM((HEADS, TOKENS), F32),
            pltpu.VMEM((TOKENS, WIDE), BF16),
            pltpu.VMEM((TOKENS, WIDE), BF16),
            dma((12,)), dma((NSLAB,)), dma((2,)), dma((4, 3)), dma((4, 3)), dma((62,)), dma((NSLAB, 2)), dma((2,)), dma((2,)),
        ],
        compiler_params=pltpu.CompilerParams(
            vmem_limit_bytes=62 << 20, collective_id=0, has_side_effects=True),
        name="layer",
    )(hidden_next, values_next, seg_next, proj_bc, proj_dt, as_row(dt_bias), as_row(decay_rate), as_row(skip_gain),
      bc_prev, dt_prev.T, seg_prev, grad_prev)


def solution(mesh):
    split = Mesh(mesh.devices.reshape(8, 2, 2, 2, 4), ("z", "xl", "c", "xh", "y"))
    tokens, both, rows = P(SEQ, None), P(SEQ, FSDP), P(SEQ + FSDP, None)
    in_specs = (tokens, both, P(), rows, rows, P(), P(), P(), tokens, both, P(), both)
    return jax.shard_map(body, mesh=split, in_specs=in_specs, out_specs=(both, both), check_vma=False)
```
